32 devices in a mesh: seq: 16 (over z, y, core), slide: 2 (over x).
Axes of the slice: x: 2, y: 2, z: 4, core: 2. Of those that a mesh axis runs over, the one named last changes fastest.
Arguments:
- layer_input: bfloat16 [2, 4096, 768], P('slide', 'seq'), may hold values from -6 to 6
- cotangent: bfloat16 [2, 4096, 768], P('slide', 'seq'), may hold values from -6 to 6
- layer_norm_gain: float32 [768], replicated, may hold values from 0.25 to 1.75
- layer_norm_bias: float32 [768], replicated, may hold values from -3 to 3
- query_key_value_weight: bfloat16 [768, 2304], replicated, may hold values from -4 to 4
- output_weight: bfloat16 [768, 768], replicated, may hold values from -0.21875 to 0.21875
Outputs:
- layer_output: bfloat16 [2, 4096, 768], P('slide', 'seq')
- input_grad: bfloat16 [2, 4096, 768], P('slide', 'seq')
- grad_qkv: float32 [768, 2304], P('seq')
- grad_out: float32 [768, 768], P('seq')
- grad_gain: float32 [768], replicated
- grad_bias: float32 [768], replicated
The draws below stay inside these ranges and needn't reach their ends.
All inputs are finite; a program needn't handle non-finite values.
Results may differ from the reference program's by a relative error of at most 0.011.
Values may be sent and summed in bfloat16 or wider, within the bound.
A program may use at most 128 MiB of HBM per device.

```python
import jax
import jax.numpy as jnp
from jax import lax

D = 768
HEADS = 12
BLOCK_TOKENS = 256
TOKENS = 4096
SLIDES = 2
N_SLIDE = 2


def draw_query_key_value_weight(key, part):
    base = jnp.clip(jax.random.normal(key, (D, 3 * D), jnp.float32), -6.0, 6.0) * D ** (-0.5)
    return base.astype(jnp.bfloat16)


def levels(key, shape, split, least, largest):
    gain = 1.0
    for axis_at, parts in split:
        draws = jax.random.uniform(jax.random.fold_in(jax.random.fold_in(key, 6), axis_at), (parts,), jnp.float32, least / len(split), largest / len(split))
        gain = gain * jnp.repeat(jnp.exp(draws), shape[axis_at] // parts).reshape((-1,) + (1,) * (len(shape) - 1 - axis_at))
    return gain


def scatter_about(rng, extent, width, limit, cuts=(), held_as=jnp.bfloat16):
    values = jax.random.normal(rng, extent, jnp.float32) * width
    if len(cuts) > 0:
        values = levels(rng, extent, cuts, -0.22, 0.18) * values
    return jnp.clip(values, min=-limit, max=limit).astype(held_as)


def setup_inputs(seed: int = 0) -> dict:
    key_list = jax.random.split(jax.random.key(seed), 7)
    layer_input = scatter_about(key_list[0], (SLIDES, TOKENS, D), 1.0, 6.0, ((0, 2), (1, 16)))
    cotangent = scatter_about(key_list[1], (SLIDES, TOKENS, D), 1.0, 6.0, ((0, 2), (1, 16)))
    layer_norm_gain = jnp.clip(1.0 + 0.15 * jax.random.normal(key_list[2], (D,), jnp.float32), 0.25, 1.75)
    layer_norm_bias = scatter_about(key_list[3], (D,), 0.5, 3.0, (), jnp.float32)
    query_key_value_weight = draw_query_key_value_weight(jax.random.fold_in(key_list[6], 71), 0)
    output_weight = scatter_about(key_list[5], (D, D), D ** -0.5, 0.21875)
    return dict(layer_input=layer_input, cotangent=cotangent, layer_norm_gain=layer_norm_gain, layer_norm_bias=layer_norm_bias, query_key_value_weight=query_key_value_weight, output_weight=output_weight)


EPS = 1e-05

def apply_layer_norm(token_rows, scale_gain, shift_bias):
    values = token_rows.astype(jnp.float32)
    centered_rows = values - lax.optimization_barrier(jnp.mean(values, axis=-1, keepdims=True))
    inverse_deviation = lax.rsqrt(lax.optimization_barrier(jnp.mean(centered_rows * centered_rows, axis=-1, keepdims=True)) + EPS)
    normalized_rows = centered_rows * inverse_deviation
    return ((normalized_rows * scale_gain + shift_bias).astype(jnp.bfloat16), normalized_rows, inverse_deviation)

def attend(qkv_self, memory_key_value, memory_present):
    token_length = qkv_self.shape[0]
    feature_width = memory_key_value.shape[1] // 2
    head_dim = feature_width // HEADS
    query = qkv_self[:, :feature_width].reshape(token_length, HEADS, head_dim).astype(jnp.float32)
    keys = jnp.concatenate([memory_key_value[:, :feature_width], qkv_self[:, feature_width:2 * feature_width]], 0)
    keys = keys.reshape(2 * token_length, HEADS, head_dim).astype(jnp.float32)
    values = jnp.concatenate([memory_key_value[:, feature_width:], qkv_self[:, 2 * feature_width:]], 0)
    values = values.reshape(2 * token_length, HEADS, head_dim).astype(jnp.float32)
    scores = jnp.einsum('qhe,khe->hqk', query, keys) * head_dim ** (-0.5)
    row_ids = lax.broadcasted_iota(jnp.int32, (token_length, 2 * token_length), 0)
    col_ids = lax.broadcasted_iota(jnp.int32, (token_length, 2 * token_length), 1)
    allowed = jnp.where(col_ids < token_length, memory_present, col_ids - token_length <= row_ids)
    scores = jnp.where(allowed[None], scores, -1e+30)
    top = lax.optimization_barrier(jnp.max(scores, axis=-1, keepdims=True))
    weights = jnp.exp(scores - top)
    probs = weights / lax.optimization_barrier(jnp.sum(weights, axis=-1, keepdims=True))
    probs_b = lax.optimization_barrier(probs.astype(jnp.bfloat16))
    mixed = jnp.einsum('hqk,khe->qhe', probs_b.astype(jnp.float32), values)
    mixed = mixed.reshape(token_length, feature_width).astype(jnp.bfloat16)
    return (mixed, probs, probs_b, query, keys, values)

def attend_back(d_mixed, probs, probs_b, query, keys, values):
    token_length, heads, head_dim = query.shape
    grad_heads = d_mixed.astype(jnp.float32).reshape(token_length, heads, head_dim)
    d_probs = jnp.einsum('qhe,khe->hqk', grad_heads, values)
    d_scores = probs * (d_probs - lax.optimization_barrier(jnp.sum(d_probs * probs, axis=-1, keepdims=True)))
    d_scores_b = lax.optimization_barrier((d_scores * head_dim ** (-0.5)).astype(jnp.bfloat16))
    d_scores_f = d_scores_b.astype(jnp.float32)
    d_query = jnp.einsum('hqk,khe->qhe', d_scores_f, keys).reshape(token_length, -1).astype(jnp.bfloat16)
    d_keys = jnp.einsum('hqk,qhe->khe', d_scores_f, query).reshape(2 * token_length, -1).astype(jnp.bfloat16)
    d_values = jnp.einsum('hqk,qhe->khe', probs_b.astype(jnp.float32), grad_heads)
    d_values = d_values.reshape(2 * token_length, -1).astype(jnp.bfloat16)
    return (d_query, d_keys, d_values)

def block_forward(token_rows, gradient_list, current_query_key_value, memory_key_value, memory_present, current_normed, current_normalized, current_inverse_deviation, query_key_value_weight, output_weight, scale_gain):
    token_length = token_rows.shape[0]
    mixed, probs, probs_b, query, keys, values = attend(current_query_key_value, memory_key_value, memory_present)
    block_output = (token_rows.astype(jnp.float32) + jnp.dot(mixed, output_weight, preferred_element_type=jnp.float32)).astype(jnp.bfloat16)
    d_mixed = jnp.dot(gradient_list, output_weight.T, preferred_element_type=jnp.float32).astype(jnp.bfloat16)
    grad_wout = jnp.dot(mixed.T, gradient_list, preferred_element_type=jnp.float32)
    d_query, d_keys, d_values = attend_back(d_mixed, probs, probs_b, query, keys, values)
    d_own = jnp.concatenate([d_query, d_keys[token_length:], d_values[token_length:]], 1)
    memory_gradient = jnp.concatenate([d_keys[:token_length], d_values[:token_length]], 1)
    grad_wqkv = jnp.dot(current_normed.T, d_own, preferred_element_type=jnp.float32)
    normed_gradient = jnp.dot(d_own, query_key_value_weight.T, preferred_element_type=jnp.float32)
    gain_gradient = lax.optimization_barrier(jnp.sum(normed_gradient * current_normalized, axis=0))
    grad_b = lax.optimization_barrier(jnp.sum(normed_gradient, axis=0))
    normalized_gradient = normed_gradient * scale_gain
    row_gradient = current_inverse_deviation * (normalized_gradient - lax.optimization_barrier(jnp.mean(normalized_gradient, axis=-1, keepdims=True)) - current_normalized * lax.optimization_barrier(jnp.mean(normalized_gradient * current_normalized, axis=-1, keepdims=True)))
    input_gradient = (gradient_list.astype(jnp.float32) + row_gradient).astype(jnp.bfloat16)
    return (block_output, input_gradient, memory_gradient, (grad_wqkv, grad_wout, gain_gradient, grad_b))

def memory_contributions(prior_normed, prior_normalized, memory_gradient, query_key_value_weight):
    feature_width = prior_normed.shape[1]
    key_value_gradient = jnp.dot(prior_normed.T, memory_gradient, preferred_element_type=jnp.float32)
    normed_gradient = jnp.dot(memory_gradient, query_key_value_weight[:, feature_width:].T, preferred_element_type=jnp.float32)
    return (key_value_gradient, lax.optimization_barrier(jnp.sum(normed_gradient * prior_normalized, axis=0)), lax.optimization_barrier(jnp.sum(normed_gradient, axis=0)))

def one_slide(token_rows, gradient_list, scale_gain, shift_bias, query_key_value_weight, output_weight):
    feature_width = token_rows.shape[1]
    count = token_rows.shape[0] // BLOCK_TOKENS
    normed_rows, normalized_rows, inverse_deviation = apply_layer_norm(token_rows, scale_gain, shift_bias)
    query_key_value = jnp.dot(normed_rows, query_key_value_weight, preferred_element_type=jnp.float32).astype(jnp.bfloat16)
    kv_all = query_key_value[:, feature_width:]
    memory_key_value = jnp.concatenate([jnp.zeros((BLOCK_TOKENS, 2 * feature_width), jnp.bfloat16), kv_all[:-BLOCK_TOKENS]], 0)
    prior_normed = jnp.concatenate([jnp.zeros((BLOCK_TOKENS, feature_width), jnp.bfloat16), normed_rows[:-BLOCK_TOKENS]], 0)
    prior_normalized = jnp.concatenate([jnp.zeros((BLOCK_TOKENS, feature_width), jnp.float32), normalized_rows[:-BLOCK_TOKENS]], 0)
    has_memory_flag = jnp.arange(count) > 0

    def block_list(array):
        return array.reshape((count, BLOCK_TOKENS) + array.shape[1:])

    def step(carry, entry_list):
        current_rows, current_gradients, current_query_key_value, current_memory, current_has_memory, current_normed, current_normalized, current_inverse_deviation, current_prior_normed, current_previous_rows = entry_list
        block_output, input_gradient, memory_gradient, term_list = block_forward(current_rows, current_gradients, current_query_key_value, current_memory, current_has_memory, current_normed, current_normalized, current_inverse_deviation, query_key_value_weight, output_weight, scale_gain)
        key_value_gradient, memory_gain, memory_bias = memory_contributions(current_prior_normed, current_previous_rows, memory_gradient, query_key_value_weight)
        acc_qkv, acc_out, acc_gain, acc_bias = carry
        acc_qkv = acc_qkv + term_list[0] + jnp.concatenate([jnp.zeros((feature_width, feature_width), jnp.float32), key_value_gradient], 1)
        return ((acc_qkv, acc_out + term_list[1], acc_gain + term_list[2] + memory_gain, acc_bias + term_list[3] + memory_bias), (block_output, input_gradient))
    init = (jnp.zeros((feature_width, 3 * feature_width), jnp.float32), jnp.zeros((feature_width, feature_width), jnp.float32), jnp.zeros((feature_width,), jnp.float32), jnp.zeros((feature_width,), jnp.float32))
    entry_list = (block_list(token_rows), block_list(gradient_list), block_list(query_key_value), block_list(memory_key_value), has_memory_flag, block_list(normed_rows), block_list(normalized_rows), block_list(inverse_deviation), block_list(prior_normed), block_list(prior_normalized))
    carry, (outputs, d_inputs) = lax.scan(step, init, entry_list)
    return (outputs.reshape(token_rows.shape), d_inputs.reshape(token_rows.shape), carry)

def reference(layer_input, cotangent, layer_norm_gain, layer_norm_bias, query_key_value_weight, output_weight):
    outputs = []
    d_inputs = []
    totals = None
    for which in range(N_SLIDE):
        block_output, input_gradient, carry = one_slide(layer_input[which], cotangent[which], layer_norm_gain, layer_norm_bias, query_key_value_weight, output_weight)
        outputs.append(block_output)
        d_inputs.append(input_gradient)
        totals = carry if totals is None else tuple((a + b for a, b in zip(totals, carry)))
    factor = 1.0 / float(N_SLIDE * layer_input.shape[1]) ** 0.5
    return (jnp.stack(outputs), jnp.stack(d_inputs), totals[0] * factor, totals[1] * factor, totals[2] * factor, totals[3] * factor)
```

```python
import functools

import jax
import jax.numpy as jnp
from jax import lax
from jax.experimental import pallas as pl
from jax.experimental.pallas import tpu as pltpu
from jax.sharding import PartitionSpec as P

HEADS = 12
EPS = 1e-05
F32 = jnp.float32
BF16 = jnp.bfloat16
NT = (((1,), (1,)), ((), ()))
VMEM_LIMIT = 60 * 1024 * 1024


def dot(a, b):
    return jnp.dot(a, b, preferred_element_type=F32)


def dot_nt(a, b):
    return lax.dot_general(a, b, NT, preferred_element_type=F32)


def norm_rows(rows, gain, shift):
    values = rows.astype(F32)
    centered = values - jnp.mean(values, axis=-1, keepdims=True)
    rstd = lax.rsqrt(jnp.mean(centered * centered, axis=-1, keepdims=True) + EPS)
    xhat = centered * rstd
    return xhat * gain + shift, xhat, rstd


def layer_kernel(
    present_ref, x_ref, xp_ref, g_ref, gain_ref, bias_ref, w_ref, wo_ref,
    out_ref, dx_ref, grads_ref, vec_ref,
    normed_t, q_s, k_s, v_s, dm_s, mixed_t, d_s,
):
    tokens, width = x_ref.shape
    head = width // HEADS
    pair = 2 * head
    groups, slides, _, span = grads_ref.shape
    gain = gain_ref[...]
    shift = bias_ref[...]

    normed_f, _, _ = norm_rows(x_ref[...], gain, shift)
    prior_f, _, _ = norm_rows(xp_ref[...], gain, shift)
    normed = normed_f.astype(BF16)
    prior = prior_f.astype(BF16)
    normed_t[:, :tokens] = normed_f.T.astype(BF16)
    normed_t[:, tokens:] = prior_f.T.astype(BF16)
    scale = head ** (-0.5)
    q_s[...] = (dot(normed, w_ref[:, :width]).astype(BF16).astype(F32) * scale).astype(BF16)
    k_s[tokens:, :] = dot(normed, w_ref[:, width : 2 * width]).astype(BF16)
    v_s[tokens:, :] = dot(normed, w_ref[:, 2 * width :]).astype(BF16)
    k_s[:tokens, :] = dot(prior, w_ref[:, width : 2 * width]).astype(BF16)
    v_s[:tokens, :] = dot(prior, w_ref[:, 2 * width :]).astype(BF16)
    dm_s[...] = dot_nt(g_ref[...], wo_ref[...]).astype(BF16)

    missing = jnp.where(present_ref[0] > 0, 0.0, -1e30).astype(F32)
    key_ids = lax.broadcasted_iota(jnp.int32, (tokens, tokens), 0)
    query_ids = lax.broadcasted_iota(jnp.int32, (tokens, tokens), 1)
    seen = key_ids <= query_ids
    lanes = lax.broadcasted_iota(jnp.int32, (tokens, pair), 1)

    for p in range(HEADS // 2):
        cols = slice(p * pair, (p + 1) * pair)
        k2 = k_s[:, cols]
        v2 = v_s[:, cols]
        k2_t = k2.astype(F32).T.astype(BF16)
        v2_t = v2.astype(F32).T.astype(BF16)
        q2 = q_s[:, cols]
        dm2 = dm_s[:, cols]
        dk = None
        dv = None
        dq_rows = []
        for h in range(2):
            mine = (lanes < head) if h == 0 else (lanes >= head)
            qh = jnp.where(mine, q2, jnp.zeros_like(q2))
            dmh = jnp.where(mine, dm2, jnp.zeros_like(dm2))
            rows = slice(h * head, (h + 1) * head)
            s = dot_nt(k2, qh)
            s_mem = s[:tokens] + missing
            s_own = jnp.where(seen, s[tokens:], -1e30)
            top = jnp.maximum(
                jnp.max(s_mem, axis=0, keepdims=True), jnp.max(s_own, axis=0, keepdims=True)
            )
            e = jnp.concatenate([jnp.exp(s_mem - top), jnp.exp(s_own - top)], 0)
            probs = e * (1.0 / jnp.sum(e, axis=0, keepdims=True))
            probs_b = probs.astype(BF16)
            mixed_t[p * pair + h * head : p * pair + (h + 1) * head, :] = dot(
                v2_t[rows], probs_b
            ).astype(BF16)
            dp = dot_nt(v2, dmh)
            ds = probs * (dp - jnp.sum(dp * probs, axis=0, keepdims=True))
            ds_b = ds.astype(BF16)
            dq_rows.append(dot(k2_t[rows], ds_b))
            dk_h = dot(ds_b, qh)
            dv_h = dot(probs_b, dmh)
            dk = dk_h if dk is None else dk + dk_h
            dv = dv_h if dv is None else dv + dv_h
        dq = jnp.concatenate(dq_rows, 0).T * scale
        kc = slice(width + p * pair, width + (p + 1) * pair)
        vc = slice(2 * width + p * pair, 2 * width + (p + 1) * pair)
        d_s[:tokens, cols] = dq.astype(BF16)
        d_s[:tokens, kc] = dk[tokens:].astype(BF16)
        d_s[tokens:, kc] = dk[:tokens].astype(BF16)
        d_s[:tokens, vc] = dv[tokens:].astype(BF16)
        d_s[tokens:, vc] = dv[:tokens].astype(BF16)

    for b in range(groups * slides):
        lo = b * span
        if lo + span <= width:
            term = dot(normed_t[:, :tokens], d_s[:tokens, lo : lo + span])
        elif lo + span <= 3 * width:
            term = dot(normed_t[...], d_s[:, lo : lo + span])
        else:
            term = dot(mixed_t[...], g_ref[:, lo - 3 * width : lo - 3 * width + span])
        grads_ref[b // slides, b % slides] = term.astype(BF16)

    mixed = mixed_t[...].astype(F32).T.astype(BF16)
    out_ref[...] = (x_ref[...].astype(F32) + dot(mixed, wo_ref[...])).astype(BF16)

    d_prior = dot_nt(d_s[tokens:, width:], w_ref[:, width:])
    _, xhat_p, _ = norm_rows(xp_ref[...], gain, shift)
    vec_ref[0:1, :] = jnp.sum(d_prior * xhat_p, axis=0, keepdims=True)
    vec_ref[1:2, :] = jnp.sum(d_prior, axis=0, keepdims=True)
    d_own = dot_nt(d_s[:tokens, :], w_ref[...])
    _, xhat, rstd = norm_rows(x_ref[...], gain, shift)
    vec_ref[0:1, :] += jnp.sum(d_own * xhat, axis=0, keepdims=True)
    vec_ref[1:2, :] += jnp.sum(d_own, axis=0, keepdims=True)
    d_hat = d_own * gain
    d_row = rstd * (
        d_hat
        - jnp.mean(d_hat, axis=-1, keepdims=True)
        - xhat * jnp.mean(d_hat * xhat, axis=-1, keepdims=True)
    )
    dx_ref[...] = (g_ref[...].astype(F32) + d_row).astype(BF16)


def radices(count):
    found = []
    while count > 1:
        if len(found) < 2 and count % 2 == 0:
            step = 2
        else:
            step = 4 if count % 4 == 0 else (2 if count % 2 == 0 else count)
        found.append(step)
        count //= step
    return found


def plan(seq_count, slides):
    digits = []
    stride = 1
    for r in radices(seq_count):
        digits.append((r, stride))
        stride *= r
    axes = list(range(len(digits) + 1))
    first, rest = axes[:1], axes[1:]
    return digits + [(slides, 0)], first, rest


def reduce_kernel(digits, orders, grads_ref, vec_ref, full_ref, total_ref, *scratch):
    stages = len(digits)
    groups = len(orders)
    recv = [list(scratch[j * stages : (j + 1) * stages]) for j in range(groups)]
    at = groups * stages
    held = [list(scratch[at + j * stages : at + (j + 1) * stages]) for j in range(groups)]
    at += groups * stages
    vec_in = scratch[at : at + stages]
    at += stages
    send_sem, recv_sem, vsend_sem, vrecv_sem, gsend_sem, grecv_sem, local_sem = scratch[at:]
    seq = lax.axis_index("seq")
    slide = lax.axis_index("slide")
    slides = digits[-1][0]

    def digit(a):
        r, stride = digits[a]
        return slide if stride == 0 else lax.rem(lax.div(seq, stride), r)

    def peer(a, k):
        r, stride = digits[a]
        here = digit(a)
        there = lax.rem(here + k, r)
        if stride == 0:
            return there, (seq, there)
        return there, (seq + (there - here) * stride, slide)

    barrier = pltpu.get_barrier_semaphore()
    count = 0
    for a in range(stages):
        for k in range(1, digits[a][0]):
            pl.semaphore_signal(
                barrier, inc=1, device_id=peer(a, k)[1], device_id_type=pl.DeviceIdType.MESH
            )
            count += 1
    pl.semaphore_wait(barrier, count)

    def index_of(j, stage, value):
        order = orders[j]
        a = order[stage]
        left = sorted(order[stage:], reverse=True)
        pos = left.index(a)
        return tuple([slice(None)] * pos) + (value,)

    offsets = [[0] for _ in range(groups)]
    base = 0
    first = []
    for a in range(stages):
        first.append(base)
        base += digits[a][0] - 1

    def source(j, stage):
        return grads_ref.at[j] if stage == 0 else held[j][stage - 1]

    def copies(j, stage):
        a = orders[j][stage]
        made = []
        for k in range(1, digits[a][0]):
            there, dev = peer(a, k)
            made.append(
                pltpu.make_async_remote_copy(
                    src_ref=source(j, stage).at[index_of(j, stage, there)],
                    dst_ref=recv[j][stage].at[k - 1],
                    send_sem=send_sem.at[j, first[a] + k - 1],
                    recv_sem=recv_sem.at[j, first[a] + k - 1],
                    device_id=dev,
                    device_id_type=pl.DeviceIdType.MESH,
                )
            )
        return made

    def vec_copies(a):
        made = []
        for k in range(1, digits[a][0]):
            _, dev = peer(a, k)
            made.append(
                pltpu.make_async_remote_copy(
                    src_ref=vec_in[a].at[digit(a)],
                    dst_ref=vec_in[a].at[digit(a)],
                    send_sem=vsend_sem.at[first[a] + k - 1],
                    recv_sem=vrecv_sem.at[first[a] + k - 1],
                    device_id=dev,
                    device_id_type=pl.DeviceIdType.MESH,
                )
            )
        return made

    def gather_copies(j):
        made = []
        for k in range(1, slides):
            _, dev = peer(stages - 1, k)
            made.append(
                pltpu.make_async_remote_copy(
                    src_ref=full_ref.at[j, slide],
                    dst_ref=full_ref.at[j, slide],
                    send_sem=gsend_sem.at[j, k - 1],
                    recv_sem=grecv_sem.at[j, k - 1],
                    device_id=dev,
                    device_id_type=pl.DeviceIdType.MESH,
                )
            )
        return made

    live = {}
    for j in range(groups):
        live[j, 0] = copies(j, 0)
        for c in live[j, 0]:
            c.start()
    vec_in[0][digit(0)] = vec_ref[...]
    vec_live = [vec_copies(0)]
    for c in vec_live[0]:
        c.start()

    for stage in range(stages):
        for j in range(groups):
            a = orders[j][stage]
            for c in live[j, stage]:
                c.wait_recv()
            total = source(j, stage)[index_of(j, stage, digit(a))].astype(F32)
            for k in range(1, digits[a][0]):
                total = total + recv[j][stage][k - 1].astype(F32)
            if stage + 1 < stages:
                held[j][stage][...] = total.astype(BF16)
                live[j, stage + 1] = copies(j, stage + 1)
                for c in live[j, stage + 1]:
                    c.start()
            else:
                full_ref[j, slide] = total.astype(BF16)
                live[j, stage + 1] = gather_copies(j)
                for c in live[j, stage + 1]:
                    c.start()
        for c in vec_live[stage]:
            c.wait_recv()
        vec_total = vec_in[stage][0]
        for i in range(1, digits[stage][0]):
            vec_total = vec_total + vec_in[stage][i]
        if stage + 1 < stages:
            vec_in[stage + 1][digit(stage + 1)] = vec_total
            vec_live.append(vec_copies(stage + 1))
            for c in vec_live[-1]:
                c.start()
        else:
            total_ref[...] = vec_total

    for j in range(groups):
        for c in live[j, stages]:
            c.wait_recv()
    for made in list(live.values()) + vec_live:
        for c in made:
            c.wait_send()


def reduce_everywhere(grads, vec, seq_count, slides):
    groups = grads.shape[0]
    digits, head, rest = plan(seq_count, slides)
    stages = len(digits)
    orders = []
    for j in range(groups):
        turn = j % len(rest)
        orders.append(head + rest[turn:] + rest[:turn])
    width, span = grads.shape[2], grads.shape[3]
    rows = width // seq_count
    dims = [digits[a][0] for a in range(stages - 2, -1, -1)]
    shaped = grads.reshape([groups, slides] + dims + [rows, span])
    recv_shapes, held_shapes = [], []
    for j in range(groups):
        for stage in range(stages):
            a = orders[j][stage]
            after = [digits[b][0] for b in sorted(orders[j][stage + 1 :], reverse=True)]
            recv_shapes.append(pltpu.VMEM(tuple([digits[a][0] - 1] + after + [rows, span]), BF16))
            held_shapes.append(pltpu.VMEM(tuple(after + [rows, span]), BF16))
    vec_shapes = [pltpu.VMEM((digits[a][0],) + vec.shape, F32) for a in range(stages)]
    links = sum(r - 1 for r, _ in digits)
    dma = pltpu.SemaphoreType.DMA
    return pl.pallas_call(
        functools.partial(reduce_kernel, digits, orders),
        out_shape=(
            jax.ShapeDtypeStruct((groups, slides, rows, span), BF16),
            jax.ShapeDtypeStruct(vec.shape, F32),
        ),
        in_specs=[pl.BlockSpec(memory_space=pltpu.VMEM)] * 2,
        out_specs=(pl.BlockSpec(memory_space=pltpu.VMEM),) * 2,
        scratch_shapes=recv_shapes + held_shapes + vec_shapes + [
            dma((groups, links)), dma((groups, links)), dma((links,)), dma((links,)),
            dma((groups, max(slides - 1, 1))), dma((groups, max(slides - 1, 1))), dma((1,)),
        ],
        compiler_params=pltpu.CompilerParams(
            collective_id=0, has_side_effects=True, vmem_limit_bytes=VMEM_LIMIT
        ),
        name="reduce_terms",
    )(shaped, vec)


def on_device(x, g, gain, shift, w, wo):
    seq_count = lax.axis_size("seq")
    slides = lax.axis_size("slide")
    x = x[0]
    g = g[0]
    tokens, width = x.shape
    route = [(i, i + 1) for i in range(seq_count - 1)]
    xp = lax.ppermute(x, "seq", route)
    present = (lax.axis_index("seq") > 0).astype(jnp.int32).reshape(1)
    groups = 4
    span = 4 * width // (groups * slides)
    vmem = pl.BlockSpec(memory_space=pltpu.VMEM)
    out, dx, grads, vec = pl.pallas_call(
        layer_kernel,
        out_shape=(
            jax.ShapeDtypeStruct((tokens, width), BF16),
            jax.ShapeDtypeStruct((tokens, width), BF16),
            jax.ShapeDtypeStruct((groups, slides, width, span), BF16),
            jax.ShapeDtypeStruct((2, width), F32),
        ),
        in_specs=[pl.BlockSpec(memory_space=pltpu.SMEM)] + [vmem] * 7,
        out_specs=(vmem,) * 4,
        scratch_shapes=[
            pltpu.VMEM((width, 2 * tokens), BF16),
            pltpu.VMEM((tokens, width), BF16),
            pltpu.VMEM((2 * tokens, width), BF16),
            pltpu.VMEM((2 * tokens, width), BF16),
            pltpu.VMEM((tokens, width), BF16),
            pltpu.VMEM((width, tokens), BF16),
            pltpu.VMEM((2 * tokens, 3 * width), BF16),
        ],
        compiler_params=pltpu.CompilerParams(vmem_limit_bytes=VMEM_LIMIT),
        name="layer",
    )(present, x, xp, g, gain.reshape(1, width), shift.reshape(1, width), w, wo)
    full, total = reduce_everywhere(grads, vec, seq_count, slides)
    factor = 1.0 / float(seq_count * slides * tokens) ** 0.5
    rows = width // seq_count
    shard = full.astype(F32) * factor
    shard = shard.transpose(2, 0, 1, 3).reshape(rows, 4 * width)
    return (
        out[None],
        dx[None],
        shard[:, : 3 * width],
        shard[:, 3 * width :],
        total[0] * factor,
        total[1] * factor,
    )


def solution(mesh):
    placed = (P("slide", "seq", None), P("slide", "seq", None), P(), P(), P(), P())
    return jax.shard_map(
        on_device,
        mesh=mesh,
        in_specs=placed,
        out_specs=(
            P("slide", "seq", None),
            P("slide", "seq", None),
            P("seq", None),
            P("seq", None),
            P(),
            P(),
        ),
        check_vma=False,
    )
```

```python
import functools

import jax
import jax.numpy as jnp
from jax import lax
from jax.experimental import pallas as pl
from jax.experimental.pallas import tpu as pltpu
from jax.sharding import PartitionSpec as P

HEADS = 12
EPS = 1e-05
F32 = jnp.float32
BF16 = jnp.bfloat16
NT = (((1,), (1,)), ((), ()))
VMEM_LIMIT = 60 * 1024 * 1024


def dot(a, b):
    return jnp.dot(a, b, preferred_element_type=F32)


def dot_nt(a, b):
    return lax.dot_general(a, b, NT, preferred_element_type=F32)


def norm_rows(rows, gain, shift):
    values = rows.astype(F32)
    centered = values - jnp.mean(values, axis=-1, keepdims=True)
    rstd = lax.rsqrt(jnp.mean(centered * centered, axis=-1, keepdims=True) + EPS)
    xhat = centered * rstd
    return xhat * gain + shift, xhat, rstd


def run_layer(
    x_ref, xp_ref, g_ref, gain_ref, bias_ref, w_ref, wo_ref,
    out_ref, dx_ref, grads_ref, vec_ref,
    normed_t, q_s, k_s, v_s, dm_s, mixed_t, d_s,
    blocks, await_prior, launch, advance,
):
    tokens, width = x_ref.shape
    head = width // HEADS
    pair = 2 * head
    slides = grads_ref.shape[1]
    span = grads_ref.shape[-1]
    dims = grads_ref.shape[2:-2]
    rows_each = grads_ref.shape[-2]
    gain = gain_ref[...]
    shift = bias_ref[...]

    normed_f, _, _ = norm_rows(x_ref[...], gain, shift)
    normed = normed_f.astype(BF16)
    normed_t[:, :tokens] = normed_f.T.astype(BF16)
    scale = head ** (-0.5)
    q_s[...] = (dot(normed, w_ref[:, :width]).astype(BF16).astype(F32) * scale).astype(BF16)
    k_s[tokens:, :] = dot(normed, w_ref[:, width : 2 * width]).astype(BF16)
    v_s[tokens:, :] = dot(normed, w_ref[:, 2 * width :]).astype(BF16)
    dm_s[...] = dot_nt(g_ref[...], wo_ref[...]).astype(BF16)
    await_prior()
    prior_f, _, _ = norm_rows(xp_ref[...], gain, shift)
    prior = prior_f.astype(BF16)
    normed_t[:, tokens:] = prior_f.T.astype(BF16)
    k_s[:tokens, :] = dot(prior, w_ref[:, width : 2 * width]).astype(BF16)
    v_s[:tokens, :] = dot(prior, w_ref[:, 2 * width :]).astype(BF16)

    def emit(j):
        for half in range(slides):
            lo = blocks[j * slides + half] * span
            if lo + span <= width:
                term = dot(normed_t[:, :tokens], d_s[:tokens, lo : lo + span])
            elif lo + span <= 3 * width:
                term = dot(normed_t[...], d_s[:, lo : lo + span])
            else:
                term = dot(mixed_t[...], g_ref[:, lo - 3 * width : lo - 3 * width + span])
            for i in range(width // rows_each):
                at, left = [], i
                for r in reversed(dims):
                    at.append(left % r)
                    left //= r
                piece = term[i * rows_each : (i + 1) * rows_each].astype(BF16)
                grads_ref[(j, half) + tuple(reversed(at))] = piece
        launch(j)

    missing = jnp.where(lax.axis_index("seq") > 0, 0.0, -1e30).astype(F32)
    key_ids = lax.broadcasted_iota(jnp.int32, (tokens, tokens), 0)
    query_ids = lax.broadcasted_iota(jnp.int32, (tokens, tokens), 1)
    seen = key_ids <= query_ids
    lanes = lax.broadcasted_iota(jnp.int32, (tokens, pair), 1)

    for p in range(HEADS // 2):
        cols = slice(p * pair, (p + 1) * pair)
        k2 = k_s[:, cols]
        v2 = v_s[:, cols]
        k2_t = k2.astype(F32).T.astype(BF16)
        v2_t = v2.astype(F32).T.astype(BF16)
        q2 = q_s[:, cols]
        dm2 = dm_s[:, cols]
        dk = None
        dv = None
        dq_rows = []
        for h in range(2):
            mine = (lanes < head) if h == 0 else (lanes >= head)
            qh = jnp.where(mine, q2, jnp.zeros_like(q2))
            dmh = jnp.where(mine, dm2, jnp.zeros_like(dm2))
            rows = slice(h * head, (h + 1) * head)
            s = dot_nt(k2, qh)
            s_mem = s[:tokens] + missing
            s_own = jnp.where(seen, s[tokens:], -1e30)
            top = jnp.maximum(
                jnp.max(s_mem, axis=0, keepdims=True), jnp.max(s_own, axis=0, keepdims=True)
            )
            e = jnp.concatenate([jnp.exp(s_mem - top), jnp.exp(s_own - top)], 0)
            probs = e * (1.0 / jnp.sum(e, axis=0, keepdims=True))
            probs_b = probs.astype(BF16)
            mixed_t[p * pair + h * head : p * pair + (h + 1) * head, :] = dot(
                v2_t[rows], probs_b
            ).astype(BF16)
            dp = dot_nt(v2, dmh)
            ds = probs * (dp - jnp.sum(dp * probs, axis=0, keepdims=True))
            ds_b = ds.astype(BF16)
            dq_rows.append(dot(k2_t[rows], ds_b))
            dk_h = dot(ds_b, qh)
            dv_h = dot(probs_b, dmh)
            dk = dk_h if dk is None else dk + dk_h
            dv = dv_h if dv is None else dv + dv_h
        dq = jnp.concatenate(dq_rows, 0).T * scale
        kc = slice(width + p * pair, width + (p + 1) * pair)
        vc = slice(2 * width + p * pair, 2 * width + (p + 1) * pair)
        d_s[:tokens, cols] = dq.astype(BF16)
        d_s[:tokens, kc] = dk[tokens:].astype(BF16)
        d_s[tokens:, kc] = dk[:tokens].astype(BF16)
        d_s[:tokens, vc] = dv[tokens:].astype(BF16)
        d_s[tokens:, vc] = dv[:tokens].astype(BF16)

        if p == HEADS // 4 - 1:
            emit(0)

    for j in range(1, grads_ref.shape[0]):
        emit(j)
        advance(j - 1)
    mixed = mixed_t[...].astype(F32).T.astype(BF16)
    out_ref[...] = (x_ref[...].astype(F32) + dot(mixed, wo_ref[...])).astype(BF16)

    advance(grads_ref.shape[0] - 1)
    d_prior = dot_nt(d_s[tokens:, width:], w_ref[:, width:])
    _, xhat_p, _ = norm_rows(xp_ref[...], gain, shift)
    vec_ref[0:1, :] = jnp.sum(d_prior * xhat_p, axis=0, keepdims=True)
    vec_ref[1:2, :] = jnp.sum(d_prior, axis=0, keepdims=True)
    d_own = dot_nt(d_s[:tokens, :], w_ref[...])
    _, xhat, rstd = norm_rows(x_ref[...], gain, shift)
    vec_ref[0:1, :] += jnp.sum(d_own * xhat, axis=0, keepdims=True)
    vec_ref[1:2, :] += jnp.sum(d_own, axis=0, keepdims=True)
    d_hat = d_own * gain
    d_row = rstd * (
        d_hat
        - jnp.mean(d_hat, axis=-1, keepdims=True)
        - xhat * jnp.mean(d_hat * xhat, axis=-1, keepdims=True)
    )
    dx_ref[...] = (g_ref[...].astype(F32) + d_row).astype(BF16)


def radices(count):
    found = []
    while count > 1:
        if len(found) < 2 and count % 2 == 0:
            step = 2
        else:
            step = 4 if count % 4 == 0 else (2 if count % 2 == 0 else count)
        found.append(step)
        count //= step
    return found


def plan(seq_count, slides):
    digits = []
    stride = 1
    for r in radices(seq_count):
        digits.append((r, stride))
        stride *= r
    axes = list(range(len(digits) + 1))
    first, rest = axes[:1], axes[1:]
    return digits + [(slides, 0)], first, rest


def sublayer_kernel(
    digits, orders, blocks, factor,
    x_ref, g_ref, gain_ref, bias_ref, w_ref, wo_ref,
    out_ref, dx_ref, qkv_ref, proj_ref, total_ref,
    grads_ref, vec_ref, full_ref, xp_ref, px_send, px_recv, *scratch,
):
    work, scratch = scratch[:7], scratch[7:]
    stages = len(digits)
    groups = len(orders)
    recv = [list(scratch[j * stages : (j + 1) * stages]) for j in range(groups)]
    at = groups * stages
    held = [list(scratch[at + j * stages : at + (j + 1) * stages]) for j in range(groups)]
    at += groups * stages
    vec_in = scratch[at : at + stages]
    at += stages
    send_sem, recv_sem, vsend_sem, vrecv_sem, gsend_sem, grecv_sem = scratch[at:]
    seq = lax.axis_index("seq")
    slide = lax.axis_index("slide")
    slides = digits[-1][0]

    def digit(a):
        r, stride = digits[a]
        return slide if stride == 0 else lax.rem(lax.div(seq, stride), r)

    def peer(a, k):
        r, stride = digits[a]
        here = digit(a)
        there = lax.rem(here + k, r)
        if stride == 0:
            return there, (seq, there)
        return there, (seq + (there - here) * stride, slide)

    barrier = pltpu.get_barrier_semaphore()
    count = 0
    for a in range(stages):
        for k in range(1, digits[a][0]):
            pl.semaphore_signal(
                barrier, inc=1, device_id=peer(a, k)[1], device_id_type=pl.DeviceIdType.MESH
            )
            count += 1
    seq_count = lax.axis_size("seq")
    ahead = lax.rem(seq + 1, seq_count)
    behind = lax.rem(seq + seq_count - 1, seq_count)
    for other in (ahead, behind):
        pl.semaphore_signal(
            barrier, inc=1, device_id=(other, slide), device_id_type=pl.DeviceIdType.MESH
        )
    pl.semaphore_wait(barrier, count + 2)
    prior_copy = pltpu.make_async_remote_copy(
        src_ref=x_ref, dst_ref=xp_ref, send_sem=px_send.at[0], recv_sem=px_recv.at[0],
        device_id=(ahead, slide), device_id_type=pl.DeviceIdType.MESH,
    )
    prior_copy.start()

    def index_of(j, stage, value):
        order = orders[j]
        a = order[stage]
        left = sorted(order[stage:], reverse=True)
        pos = left.index(a)
        return tuple([slice(None)] * pos) + (value,)

    offsets = [[0] for _ in range(groups)]
    base = 0
    first = []
    for a in range(stages):
        first.append(base)
        base += digits[a][0] - 1

    def source(j, stage):
        return grads_ref.at[j] if stage == 0 else held[j][stage - 1]

    def copies(j, stage):
        a = orders[j][stage]
        made = []
        for k in range(1, digits[a][0]):
            there, dev = peer(a, k)
            made.append(
                pltpu.make_async_remote_copy(
                    src_ref=source(j, stage).at[index_of(j, stage, there)],
                    dst_ref=recv[j][stage].at[k - 1],
                    send_sem=send_sem.at[j, first[a] + k - 1],
                    recv_sem=recv_sem.at[j, first[a] + k - 1],
                    device_id=dev,
                    device_id_type=pl.DeviceIdType.MESH,
                )
            )
        return made

    def vec_copies(a):
        made = []
        for k in range(1, digits[a][0]):
            _, dev = peer(a, k)
            made.append(
                pltpu.make_async_remote_copy(
                    src_ref=vec_in[a].at[digit(a)],
                    dst_ref=vec_in[a].at[digit(a)],
                    send_sem=vsend_sem.at[first[a] + k - 1],
                    recv_sem=vrecv_sem.at[first[a] + k - 1],
                    device_id=dev,
                    device_id_type=pl.DeviceIdType.MESH,
                )
            )
        return made

    def gather_copies(j):
        made = []
        for k in range(1, slides):
            _, dev = peer(stages - 1, k)
            made.append(
                pltpu.make_async_remote_copy(
                    src_ref=full_ref.at[j, slide],
                    dst_ref=full_ref.at[j, slide],
                    send_sem=gsend_sem.at[j, k - 1],
                    recv_sem=grecv_sem.at[j, k - 1],
                    device_id=dev,
                    device_id_type=pl.DeviceIdType.MESH,
                )
            )
        return made

    live = {}
    vec_live = []

    def launch(j):
        live[j, 0] = copies(j, 0)
        for c in live[j, 0]:
            c.start()

    def step(stage, j):
        a = orders[j][stage]
        for c in live[j, stage]:
            c.wait_recv()
        total = source(j, stage)[index_of(j, stage, digit(a))].astype(F32)
        for k in range(1, digits[a][0]):
            total = total + recv[j][stage][k - 1].astype(F32)
        if stage + 1 < stages:
            held[j][stage][...] = total.astype(BF16)
            live[j, stage + 1] = copies(j, stage + 1)
        else:
            full_ref[j, slide] = total.astype(BF16)
            live[j, stage + 1] = gather_copies(j)
        for c in live[j, stage + 1]:
            c.start()

    def advance(diagonal):
        for j in range(groups):
            if 0 <= diagonal - j < stages:
                step(diagonal - j, j)

    def vec_start(stage, value):
        vec_in[stage][digit(stage)] = value
        vec_live.append(vec_copies(stage))
        for c in vec_live[-1]:
            c.start()

    def vec_step(stage):
        for c in vec_live[stage]:
            c.wait_recv()
        value = vec_in[stage][0]
        for i in range(1, digits[stage][0]):
            value = value + vec_in[stage][i]
        if stage + 1 < stages:
            vec_start(stage + 1, value)
        else:
            total_ref[...] = value

    run_layer(
        x_ref, xp_ref, g_ref, gain_ref, bias_ref, w_ref, wo_ref, out_ref, dx_ref,
        grads_ref, vec_ref, *work, blocks, prior_copy.wait_recv, launch, advance,
    )
    vec_start(0, vec_ref[...])
    done = 0
    for diagonal in range(groups, stages + groups - 1):
        advance(diagonal)
        if done < stages:
            vec_step(done)
            done += 1
    for stage in range(done, stages):
        vec_step(stage)
    span = full_ref.shape[-1]
    for j in range(groups):
        for c in live[j, stages]:
            c.wait_recv()
        for half in range(slides):
            lo = blocks[j * slides + half] * span
            value = full_ref[j, half].astype(F32) * factor
            if lo < qkv_ref.shape[1]:
                qkv_ref[:, lo : lo + span] = value
            else:
                lo -= qkv_ref.shape[1]
                proj_ref[:, lo : lo + span] = value
    prior_copy.wait_send()
    for made in list(live.values()) + vec_live:
        for c in made:
            c.wait_send()


def on_device(x, g, gain, shift, w, wo):
    seq_count = lax.axis_size("seq")
    slides = lax.axis_size("slide")
    tokens, width = x.shape[1:]
    groups = 8 // slides
    blocks = (0, 2, 4, 1, 3, 5, 6, 7)
    span = width // 2
    factor = 1.0 / float(seq_count * slides * tokens) ** 0.5
    digits, head, rest = plan(seq_count, slides)
    stages = len(digits)
    near, far, last = rest[0], rest[1:-1], rest[-1]
    kinds = [[last, near] + far, [near, last] + far, [last] + far + [near], [near] + far + [last]]
    orders = [head + kinds[j % len(kinds)] for j in range(groups)]
    rows = width // seq_count
    dims = [digits[a][0] for a in range(stages - 2, -1, -1)]
    recv_shapes, held_shapes = [], []
    for j in range(groups):
        for stage in range(stages):
            a = orders[j][stage]
            after = [digits[b][0] for b in sorted(orders[j][stage + 1 :], reverse=True)]
            recv_shapes.append(pltpu.VMEM(tuple([digits[a][0] - 1] + after + [rows, span]), BF16))
            held_shapes.append(pltpu.VMEM(tuple(after + [rows, span]), BF16))
    vec_shapes = [pltpu.VMEM((digits[a][0], 2, width), F32) for a in range(stages)]
    links = sum(r - 1 for r, _ in digits)
    dma = pltpu.SemaphoreType.DMA
    vmem = pl.BlockSpec(memory_space=pltpu.VMEM)
    out, dx, qkv, proj, total = pl.pallas_call(
        functools.partial(sublayer_kernel, digits, orders, blocks, factor),
        out_shape=(
            jax.ShapeDtypeStruct((tokens, width), BF16),
            jax.ShapeDtypeStruct((tokens, width), BF16),
            jax.ShapeDtypeStruct((rows, 3 * width), F32),
            jax.ShapeDtypeStruct((rows, width), F32),
            jax.ShapeDtypeStruct((2, width), F32),
        ),
        in_specs=[vmem] * 6,
        out_specs=(vmem,) * 5,
        scratch_shapes=[
            pltpu.VMEM(tuple([groups, slides] + dims + [rows, span]), BF16),
            pltpu.VMEM((2, width), F32),
            pltpu.VMEM((groups, slides, rows, span), BF16),
            pltpu.VMEM((tokens, width), BF16),
            dma((1,)),
            dma((1,)),
            pltpu.VMEM((width, 2 * tokens), BF16),
            pltpu.VMEM((tokens, width), BF16),
            pltpu.VMEM((2 * tokens, width), BF16),
            pltpu.VMEM((2 * tokens, width), BF16),
            pltpu.VMEM((tokens, width), BF16),
            pltpu.VMEM((width, tokens), BF16),
            pltpu.VMEM((2 * tokens, 3 * width), BF16),
        ] + recv_shapes + held_shapes + vec_shapes + [
            dma((groups, links)), dma((groups, links)), dma((links,)), dma((links,)),
            dma((groups, max(slides - 1, 1))), dma((groups, max(slides - 1, 1))),
        ],
        compiler_params=pltpu.CompilerParams(
            collective_id=0, has_side_effects=True, vmem_limit_bytes=VMEM_LIMIT
        ),
        name="sublayer",
    )(x[0], g[0], gain.reshape(1, width), shift.reshape(1, width), w, wo)
    return (out[None], dx[None], qkv, proj, total[0] * factor, total[1] * factor)


def solution(mesh):
    placed = (P("slide", "seq", None), P("slide", "seq", None), P(), P(), P(), P())
    return jax.shard_map(
        on_device,
        mesh=mesh,
        in_specs=placed,
        out_specs=(
            P("slide", "seq", None),
            P("slide", "seq", None),
            P("seq", None),
            P("seq", None),
            P(),
            P(),
        ),
        check_vma=False,
    )
```
